512 devices in a mesh: doc: 8 (over x, core), seq: 64 (over z, y).
Axes of the slice: x: 4, y: 4, z: 16, core: 2. Of those that a mesh axis runs over, the one named last changes fastest.
Arguments:
- queries: bfloat16 [65536, 1792], P(('doc', 'seq')), parts along dimension 0, may hold values from -5 to 5
- keys: bfloat16 [65536, 256], P(('doc', 'seq')), parts along dimension 0, may hold values from -5 to 5
- values: bfloat16 [65536, 256], P(('doc', 'seq')), parts along dimension 0, may hold values from -6 to 6
- doc_length: int32 [8], P('doc'), parts along dimension 0, may hold values from 4096 to 8192
- sink_pos: int32 [32], P('doc'), parts along dimension 0, may hold values from 0 to 127, as said below
Outputs:
- attended: bfloat16 [65536, 1792], P(('doc', 'seq')), parts along dimension 0
- row_lse: float32 [14, 65536], P(None, ('doc', 'seq')), parts along dimension 1
- sink_mass: float32 [14, 65536], P(None, ('doc', 'seq')), parts along dimension 1
- head_lse: float32 [112], P('doc'), parts along dimension 0
- head_sink: float32 [112], P('doc'), parts along dimension 0
The draws below stay inside these ranges and needn't reach their ends.
There are 8 independent parts, one for each index of `doc`. The reference program is written for one: setup_inputs(seed, part) draws one part's arguments, and reference() takes and returns one part's arrays. A program takes and returns all parts, laid end to end along the dimension named above; each array names one. Nothing has to cross between parts.
Inputs may be any that keep to these rules, and one draw needn't show every extreme that they name: `sink_pos`: 4 distinct positions within the document's first 128 tokens; positions 0 and 127 are always among them. Positions from doc_length up to 8192 are padding.
All inputs are finite; a program needn't handle non-finite values.
Results may differ from the reference program's by a relative error of at most 0.009.
Values may be sent and summed in bfloat16 or wider, within the bound.
A program may use at most 64 MiB of HBM per device.

```python
import jax
import jax.numpy as jnp
from jax import lax

QUERY_HEADS = 14
KEY_VALUE_HEADS = 2
HEAD_DIMENSION = 128
NSINK = 4
S_DEV = 128
PADDED_LENGTH = 8192


def draw_queries(key, part):
    query_group_width = QUERY_HEADS // KEY_VALUE_HEADS
    unsharded_result = jnp.clip(jax.random.normal(jax.random.fold_in(key, 11), (PADDED_LENGTH, KEY_VALUE_HEADS, query_group_width, HEAD_DIMENSION), jnp.float32), -5.0, 5.0)
    return unsharded_result.reshape(PADDED_LENGTH, QUERY_HEADS * HEAD_DIMENSION).astype(jnp.bfloat16)


def draw_keys(key, part):
    unsharded_result = jnp.clip(jax.random.normal(jax.random.fold_in(key, 13), (PADDED_LENGTH, KEY_VALUE_HEADS, HEAD_DIMENSION), jnp.float32), -5.0, 5.0)
    return unsharded_result.reshape(PADDED_LENGTH, KEY_VALUE_HEADS * HEAD_DIMENSION).astype(jnp.bfloat16)


def draw_sink_pos(key, part):
    order = jax.random.permutation(jax.random.fold_in(key, 17), S_DEV - 2)
    middle = order[:NSINK - 2].astype(jnp.int32) + 1
    first = jnp.zeros((1,), jnp.int32)
    last = jnp.full((1,), S_DEV - 1, jnp.int32)
    return jnp.concatenate([first, middle, last]).astype(jnp.int32)


def level_of(key, extent, split, low, top_value):
    loudness, own = 1.0, jax.random.fold_in(key, 6)
    for dim, shards_of in split:
        draws = jnp.exp(jax.random.uniform(jax.random.fold_in(own, dim), (shards_of,), jnp.float32, low / len(split), top_value / len(split)))
        loudness = loudness * jnp.repeat(draws, extent[dim] // shards_of).reshape([-1 if axis == dim else 1 for axis in range(len(extent))])
    return loudness


def scatter_about(rng, extent, deviation, most, pieces=(), kind=jnp.bfloat16):
    drawn = jax.random.normal(rng, extent, jnp.float32) * deviation
    if len(pieces) > 0:
        drawn = level_of(rng, extent, pieces, -0.22, 0.18) * drawn
    return jnp.clip(drawn, min=-most, max=most).astype(kind)


def setup_inputs(seed: int = 0, part: int = 0) -> dict:
    splits = jax.random.split(jax.random.key(seed), 6)
    own_keys = jax.random.split(jax.random.fold_in(splits[5], part), 6)
    return {
        "queries": draw_queries(jax.random.fold_in(jax.random.fold_in(splits[5], part), 71), part),
        "keys": draw_keys(jax.random.fold_in(jax.random.fold_in(splits[5], part), 71), part),
        "values": scatter_about(own_keys[2], (PADDED_LENGTH, KEY_VALUE_HEADS * HEAD_DIMENSION), 1.0, 6.0, ((0, 64),)),
        "doc_length": jax.random.randint(own_keys[3], (1,), PADDED_LENGTH // 2, PADDED_LENGTH + 1).astype(jnp.int32),
        "sink_pos": draw_sink_pos(jax.random.fold_in(jax.random.fold_in(splits[5], part), 71), part),
    }


def reference(queries, keys, values, doc_length, sink_pos):
    query_group_width = QUERY_HEADS // KEY_VALUE_HEADS
    length = doc_length[0]
    key_float = keys.reshape(PADDED_LENGTH, KEY_VALUE_HEADS, HEAD_DIMENSION).astype(jnp.float32)
    value_float = values.reshape(PADDED_LENGTH, KEY_VALUE_HEADS, HEAD_DIMENSION).astype(jnp.float32)
    key_pos = jnp.arange(PADDED_LENGTH, dtype=jnp.int32)
    is_sink = jnp.any(key_pos[:, None] == sink_pos[None, :], axis=1)
    rows_per_block = min(512, PADDED_LENGTH)
    block_count = PADDED_LENGTH // rows_per_block
    score_scale = HEAD_DIMENSION ** -0.5

    def one_block(block_index):
        first = (block_index * rows_per_block).astype(jnp.int32)
        query_float = lax.dynamic_slice_in_dim(queries, first, rows_per_block, 0)
        query_float = query_float.reshape(rows_per_block, KEY_VALUE_HEADS, query_group_width, HEAD_DIMENSION).astype(jnp.float32)
        scores = jnp.einsum("sgcd,pgd->gcsp", query_float, key_float, precision=lax.Precision.HIGHEST) * score_scale
        query_pos = first + jnp.arange(rows_per_block, dtype=jnp.int32)
        allowed = (key_pos[None, :] <= query_pos[:, None]) & (key_pos[None, :] < length)
        masked = jnp.where(allowed, scores, -jnp.inf)
        peak = jnp.max(masked, axis=-1, keepdims=True)
        row_lse = peak[..., 0] + jnp.log(jnp.sum(jnp.exp(masked - peak), axis=-1))
        probs = jnp.exp(masked - row_lse[..., None])
        sink_mass = jnp.sum(jnp.where(is_sink, probs, 0.0), axis=-1)
        rounded = lax.optimization_barrier(probs.astype(jnp.bfloat16)).astype(jnp.float32)
        attended = jnp.einsum("gcsp,pgd->sgcd", rounded, value_float, precision=lax.Precision.HIGHEST)
        attended = attended.reshape(rows_per_block, QUERY_HEADS * HEAD_DIMENSION)
        live_rows = query_pos < length
        attended = jnp.where(live_rows[:, None], attended, 0.0).astype(jnp.bfloat16)
        row_lse = jnp.where(live_rows[None, :], row_lse.reshape(QUERY_HEADS, rows_per_block), 0.0)
        sink_mass = jnp.where(live_rows[None, :], sink_mass.reshape(QUERY_HEADS, rows_per_block), 0.0)
        return attended, row_lse, sink_mass

    attended, row_lse, sink_mass = lax.map(one_block, jnp.arange(block_count, dtype=jnp.int32))
    attended = attended.reshape(PADDED_LENGTH, QUERY_HEADS * HEAD_DIMENSION)
    row_lse = row_lse.transpose(1, 0, 2).reshape(QUERY_HEADS, PADDED_LENGTH)
    sink_mass = sink_mass.transpose(1, 0, 2).reshape(QUERY_HEADS, PADDED_LENGTH)
    doc_count = length.astype(jnp.float32)
    head_lse = jnp.sum(row_lse, axis=1) / doc_count
    head_sink = jnp.sum(sink_mass, axis=1) / doc_count
    return (attended, row_lse, sink_mass, head_lse, head_sink)
```

```python
import functools

import jax
import jax.numpy as jnp
from jax import lax
from jax.experimental import pallas as pl
from jax.experimental.pallas import tpu as pltpu
from jax.sharding import PartitionSpec as P

D = 128
ROWS = 128
GROUP = 7
HALF = GROUP * D
FLAT = GROUP * ROWS
YS = 4
LOG2E = 1.4426950408889634
LN2 = 0.6931471805599453
SCALE = LOG2E * D**-0.5
NEG = -1e30
MESH = pl.DeviceIdType.MESH
TILES = ((0, 2), (2, 4), (4, 7))
OWN, PART, HEAD, DIAG = range(4)
Q_HEAD_0, Q_PART, Q_HEAD_1, Q_DIAG = 2, 3, 4, 8


def kernel(
    zs, q_ref, k_ref, v_ref, len_ref, sink_ref,
    att_ref, lse_ref, mass_ref, tot_ref,
    kv, xbuf, qbuf, qsend, acc, l_acc, m_acc, obuf, rx, fin, fin_rx, statb, stats, red, wts,
    ring_send, ring_recv, x_send, x_recv, q_send, q_recv, st_send, st_recv, o_send, o_recv,
    red_send, red_recv,
):
    fs = zs // 2
    seq = lax.axis_index("seq")
    z, y = seq // YS, seq % YS
    head = ((y + 1) // 2) % 2
    part = y // 2
    y_head = y + 1 - 2 * (y % 2)
    y_part = 3 - y
    y_diag = y_part + 1 - 2 * (y_part % 2)
    right, left = (z + 1) % zs, (z + zs - 1) % zs
    base = z * YS

    def at(zz, yy):
        return {"seq": zz * YS + yy}

    def remote(src, dst, send, recv, target):
        return pltpu.make_async_remote_copy(
            src_ref=src, dst_ref=dst, send_sem=send, recv_sem=recv, device_id=target, device_id_type=MESH
        )

    first = head == 0
    mine = y % 2
    for i, ref in enumerate((k_ref, v_ref)):
        lo, hi = ref[:, :D], ref[:, D:]
        kv[z, mine, i] = jnp.where(first, lo, hi)
        xbuf[i] = jnp.where(first, hi, lo)
    qlo, qhi = q_ref[:, :HALF], q_ref[:, HALF:]
    qbuf[OWN] = jnp.where(first, qlo, qhi)
    qsend[...] = jnp.where(first, qhi, qlo)

    barrier = pltpu.get_barrier_semaphore()
    for target in (at(right, y), at(left, y), at(z, y_head), at(z, y_part), at(z, y_diag)):
        pl.semaphore_signal(barrier, inc=1, device_id=target, device_id_type=MESH)
    pl.semaphore_wait(barrier, 5)

    def hop(direction, s, c, plane):
        return remote(
            kv.at[plane, c], kv.at[plane, c],
            ring_send.at[direction, s, c], ring_recv.at[direction, s + 1, c],
            at(right if direction == 0 else left, y),
        )

    def arrived(direction, s, c, plane):
        return remote(
            kv.at[plane, c], kv.at[plane, c],
            ring_send.at[direction, s - 1, c], ring_recv.at[direction, s, c],
            at(right if direction == 0 else left, y),
        )

    def q_copy(k):
        lo, hi = slice(0, 4 * D), slice(4 * D, HALF)
        src, dst, target = (
            (qsend.at[:, lo], qbuf.at[HEAD, :, lo], y_head),
            (qsend.at[:, hi], qbuf.at[HEAD, :, hi], y_head),
            (qbuf.at[OWN], qbuf.at[PART], y_part),
            (qbuf.at[HEAD, :, lo], qbuf.at[DIAG, :, lo], y_part),
            (qbuf.at[HEAD, :, hi], qbuf.at[DIAG, :, hi], y_part),
        )[k]
        return remote(src, dst, q_send.at[k], q_recv.at[k], at(z, target))

    other = 1 - mine
    to_head = remote(xbuf, kv.at[z, mine], x_send, x_recv, at(z, y_head))
    from_head = remote(xbuf, kv.at[z, other], x_send, x_recv, at(z, y_head))
    to_head.start()
    hop(0, 0, mine, z).start()
    hop(1, 0, mine, z).start()
    q_copy(0).start()
    q_copy(1).start()
    q_copy(2).start()
    from_head.wait_recv()
    hop(0, 0, other, z).start()
    hop(1, 0, other, z).start()

    def owner(b):
        return jnp.where(b == OWN, y, jnp.where(b == PART, y_part, jnp.where(b == HEAD, y_head, y_diag)))

    def scores(b, heads, key_mat):
        lo, hi = heads
        rows = jnp.concatenate([qbuf[b, :, j * D : (j + 1) * D] for j in range(lo, hi)], axis=0)
        s = lax.dot_general(rows, key_mat, (((1,), (1,)), ((), ())), preferred_element_type=jnp.float32)
        return [s[:, j : j + D] * SCALE for j in range(0, key_mat.shape[0], D)]

    def top(groups):
        best = groups[0]
        for g in groups[1:]:
            best = jnp.maximum(best, g)
        return jnp.broadcast_to(jnp.max(best, axis=1, keepdims=True), best.shape)

    def total(groups):
        out = groups[0]
        for g in groups[1:]:
            out = out + g
        return out

    def first_unit(b):
        key_mat = jnp.concatenate([kv[z, 0, 0], kv[z, 1, 0]], axis=0)
        val_mat = jnp.concatenate([kv[z, 0, 1], kv[z, 1, 1]], axis=0)
        for heads in TILES:
            n = (heads[1] - heads[0]) * ROWS
            rows = pl.ds(heads[0] * ROWS, n)
            gs = scores(b, heads, key_mat)
            row = lax.broadcasted_iota(jnp.int32, (n, D), 0) % ROWS + owner(b) * ROWS
            lane = lax.broadcasted_iota(jnp.int32, (n, D), 1) + part * (2 * ROWS)
            ok = [lane + j * D <= row for j in range(2)]
            gs = [jnp.where(o, g, 2 * NEG) for o, g in zip(ok, gs)]
            m = jnp.maximum(top(gs), NEG)
            ps = [jnp.exp2(g - m) for g in gs]
            m_acc[b, rows] = m
            l_acc[b, rows] = total(ps)
            acc[b, rows] = jnp.dot(
                jnp.concatenate(ps, axis=1).astype(jnp.bfloat16), val_mat, preferred_element_type=jnp.float32
            )

    def later_unit(b, planes):
        key_mat = jnp.concatenate([kv[p, a, 0] for p in planes for a in range(2)], axis=0)
        val_mat = jnp.concatenate([kv[p, a, 1] for p in planes for a in range(2)], axis=0)
        for heads in TILES:
            rows = pl.ds(heads[0] * ROWS, (heads[1] - heads[0]) * ROWS)
            gs = scores(b, heads, key_mat)
            old = m_acc[b, rows]
            m = jnp.maximum(old, top(gs))
            alpha = jnp.exp2(old - m)
            ps = [jnp.exp2(g - m) for g in gs]
            m_acc[b, rows] = m
            l_acc[b, rows] = l_acc[b, rows] * alpha + total(ps)
            acc[b, rows] = acc[b, rows] * alpha + jnp.dot(
                jnp.concatenate(ps, axis=1).astype(jnp.bfloat16), val_mat, preferred_element_type=jnp.float32
            )

    def unit(b, s):
        ahead, behind = (z + zs - s) % zs, (z + s) % zs
        both = (z + s >= zs) & (s < fs)
        single = (z >= s) & jnp.logical_not(both) & (s > 0)

        @pl.when(s == 0)
        def _():
            first_unit(b)

        @pl.when(both)
        def _():
            later_unit(b, (ahead, behind))

        @pl.when(single)
        def _():
            later_unit(b, (ahead,))

    lane_id = lax.broadcasted_iota(jnp.int32, (ROWS, D), 1)

    def sink_pass(b):
        spot = lax.broadcasted_iota(jnp.int32, (ROWS, D), 1)
        hit = spot == sink_ref[0]
        for n in range(1, 4):
            hit = hit | (spot == sink_ref[n])
        row = lax.broadcasted_iota(jnp.int32, (ROWS, D), 0) + base * ROWS + owner(b) * ROWS
        hit = hit & (spot <= row)
        out = jnp.zeros((ROWS, D), jnp.float32)
        key_mat = kv[0, 0, 0]
        for heads in TILES:
            (s,) = scores(b, heads, key_mat)
            for j in range(heads[1] - heads[0]):
                g = jnp.where(hit, s[j * ROWS : (j + 1) * ROWS], 2 * NEG)
                m = jnp.max(g, axis=1, keepdims=True)
                r = m + jnp.log2(jnp.sum(jnp.exp2(g - m), axis=1, keepdims=True))
                out = jnp.where(lane_id == 8 + heads[0] + j, r, out)
        statb[b] = out

    reach = jnp.where(z <= fs, z, zs - z)
    early = min(max(2 * fs - 4, Q_DIAG), 2 * fs - 1)
    sink_half = jnp.where(2 * reach - 1 <= early, early, 2 * fs - 1)

    def count(b, h):
        own = 1 + (h + 1) // 2
        late = 1 + h // 2
        begun = lambda start, cap: jnp.minimum(cap, jnp.maximum(0, 2 * (h + 1 - start)))
        last = h >= 2 * fs - 1
        n = jnp.where(
            b == OWN, jnp.where(h < 0, 0, own),
            jnp.where(b == PART, begun(Q_PART, own), jnp.where(b == HEAD, begun(Q_HEAD_1, late), begun(Q_DIAG, late))),
        )
        return jnp.where(last, fs + 1, n)

    q_head_0, q_part, q_head_1, q_diag = (min(t, 2 * fs - 1) for t in (Q_HEAD_0, Q_PART, Q_HEAD_1, Q_DIAG))

    def half_step(h, carry):
        s = 1 + h // 2
        c = (mine + h) % 2
        ahead, behind = (z + zs - s) % zs, (z + s) % zs
        arrived(0, s, c, ahead).wait_recv()

        @pl.when(s < fs)
        def _():
            hop(0, s, c, ahead).start()

            arrived(1, s, c, behind).wait_recv()

        @pl.when(s < fs - 1)
        def _():
            hop(1, s, c, behind).start()

        @pl.when(h == q_head_0)
        def _():
            q_copy(0).wait_recv()
            q_copy(3).start()

        @pl.when(h == q_part)
        def _():
            q_copy(2).wait_recv()

        @pl.when(h == q_head_1)
        def _():
            q_copy(1).wait_recv()
            q_copy(4).start()

        @pl.when(h == q_diag)
        def _():
            q_copy(3).wait_recv()
            q_copy(4).wait_recv()

        def block(i, carry):
            b = 3 - i
            lo = jnp.where(h == 0, 0, count(b, h - 1))

            def one(u, carry):
                unit(b, u)
                return carry

            return lax.fori_loop(lo, count(b, h), one, carry)

        lax.fori_loop(0, 4, block, 0)

        @pl.when((h == sink_half) & (part == 0))
        def _():
            def one(b, carry):
                sink_pass(b)
                return carry

            lax.fori_loop(0, 4, one, 0)

        return carry

    @pl.when(part != 0)
    def _():
        statb[...] = jnp.zeros_like(statb)

    lax.fori_loop(0, 2 * fs, half_step, 0)

    def norm(b, carry):
        out = statb[b]
        for j in range(GROUP):
            rows = pl.ds(j * ROWS, ROWS)
            l = jnp.sum(l_acc[b, rows], axis=1, keepdims=True)
            r = jnp.where(l > 0, m_acc[b, rows] + jnp.log2(l), NEG)
            out = jnp.where(lane_id == j, r, out)
            l_acc[b, rows] = jnp.broadcast_to(jnp.where(l > 0, 1.0 / l, 0.0), (ROWS, D))
        out = jnp.where((lane_id % 8 == 7) | (lane_id >= 16), 0.0, out)
        stats[y, owner(b)] = out.T[:16]
        return carry

    lax.fori_loop(0, 4, norm, 0)

    def stat_copy(k, sender):
        target = (y_head, y_part, y_diag)[k]
        return remote(stats.at[sender], stats.at[sender], st_send.at[k], st_recv.at[k], at(z, target))

    def out_block(b, i):
        for j in range(GROUP):
            rows = pl.ds(j * ROWS, ROWS)
            obuf[i, :, j * D : (j + 1) * D] = (acc[b, rows] * l_acc[b, rows]).astype(jnp.bfloat16)

    def o_copy(k):
        src, dst, target = (
            (obuf.at[0], rx.at[0], y_part),
            (obuf.at[1], rx.at[1], y_part),
            (fin, fin_rx, y_head),
        )[k]
        return remote(src, dst, o_send.at[k], o_recv.at[k], at(z, target))

    out_block(DIAG, 0)
    for k in (1, 0, 2):
        stat_copy(k, y).start()
    out_block(PART, 1)
    o_copy(0).start()
    for k, sender in enumerate((y_head, y_part, y_diag)):
        stat_copy(k, sender).wait_recv()
    o_copy(1).start()

    length = len_ref[0]
    sums = [jnp.zeros((8, D), jnp.float32) for _ in range(4)]
    for blk in range(YS):
        pos = lax.broadcasted_iota(jnp.int32, (8, D), 1) + (base + blk) * ROWS
        live = pos < length
        for g, (a, b) in enumerate(((0, 3), (1, 2))):
            x0, x1 = stats[a, blk, 0:8], stats[b, blk, 0:8]
            m = jnp.maximum(x0, x1)
            full = m + jnp.log2(jnp.exp2(x0 - m) + jnp.exp2(x1 - m))
            mass = jnp.where(live, jnp.exp2(stats[a, blk, 8:16] - full), 0.0)
            nat = jnp.where(live, full * LN2, 0.0)
            sums[g] = sums[g] + nat
            sums[2 + g] = sums[2 + g] + mass

            @pl.when(y == blk)
            def _():
                lse_ref[g * GROUP : (g + 1) * GROUP, :] = nat[:GROUP]
                mass_ref[g * GROUP : (g + 1) * GROUP, :] = mass[:GROUP]

    lane8 = lax.broadcasted_iota(jnp.int32, (8, D), 1)
    sub8 = lax.broadcasted_iota(jnp.int32, (8, D), 0)
    line = jnp.zeros((8, D), jnp.float32)
    for i, block_sum in enumerate(sums):
        col = jnp.where(sub8 < GROUP, jnp.sum(block_sum, axis=1, keepdims=True), 0.0)
        line = line + jnp.where(lane8 == sub8 + GROUP * i, col, 0.0)
    red[z] = jnp.sum(line, axis=0, keepdims=True)

    def weights(own):
        pos = lax.broadcasted_iota(jnp.int32, (8, D), 1) + (base + own) * ROWS
        live = pos < length
        x0 = stats[y, own, 0:8]
        x1 = stats[y_part, own, 0:8]
        m = jnp.maximum(x0, x1)
        full = m + jnp.log2(jnp.exp2(x0 - m) + jnp.exp2(x1 - m))
        return [jnp.where(live, jnp.exp2(x - full), 0.0) for x in (x0, x1)]

    pad = jnp.zeros((D - 32, D), jnp.float32)
    wts[...] = jnp.concatenate([*weights(y), *weights(y_head), pad], axis=0).T

    def red_copy(k):
        return remote(red.at[z], red.at[z], red_send.at[k], red_recv.at[z], at((z + k) % zs, y))

    def red_start(k, carry):
        red_copy(k).start()
        return carry

    lax.fori_loop(1, zs, red_start, 0)

    def merged(b, i, j, w):
        rows = pl.ds(j * ROWS, ROWS)
        mine_o = acc[b, rows] * (l_acc[b, rows] * wts[:, w + j : w + j + 1])
        their_o = rx[i, :, j * D : (j + 1) * D].astype(jnp.float32) * wts[:, w + 8 + j : w + 9 + j]
        return (mine_o + their_o).astype(jnp.bfloat16)

    o_copy(0).wait_recv()
    for j in range(GROUP):
        fin[:, j * D : (j + 1) * D] = merged(HEAD, 0, j, 16)
    o_copy(2).start()
    o_copy(1).wait_recv()
    for j in range(GROUP):
        tile = merged(OWN, 1, j, 0)
        obuf[2, :, j * D : (j + 1) * D] = tile
    o_copy(2).wait_recv()
    att_ref[:, :HALF] = jnp.where(first, obuf[2], fin_rx[...])
    att_ref[:, HALF:] = jnp.where(first, fin_rx[...], obuf[2])

    def red_wait(k, carry):
        src = (z + k) % zs
        remote(red.at[src], red.at[src], red_send.at[k], red_recv.at[src], at(src, y)).wait_recv()
        return carry

    lax.fori_loop(1, zs, red_wait, 0)
    result = red[0]
    for i in range(1, zs):
        result = result + red[i]
    tot_ref[...] = result / length.astype(jnp.float32)

    to_head.wait_send()
    for k in range(5):
        q_copy(k).wait_send()
    for k in range(3):
        stat_copy(k, y).wait_send()
        o_copy(k).wait_send()

    def drain(k, carry):
        red_copy(k).wait_send()
        return carry

    lax.fori_loop(1, zs, drain, 0)

    def ring_drain(s, carry):
        for c in range(2):
            hop(0, s, c, (z + zs - s) % zs).wait_send()

            @pl.when(s < fs - 1)
            def _():
                hop(1, s, c, (z + s) % zs).wait_send()

        return carry

    lax.fori_loop(0, fs, ring_drain, 0)


def body(queries, keys, values, doc_length, sink_pos, zs):
    vmem = pl.BlockSpec(memory_space=pltpu.VMEM)
    smem = pl.BlockSpec(memory_space=pltpu.SMEM)
    fs = zs // 2
    bf16, f32 = jnp.bfloat16, jnp.float32
    dma = pltpu.SemaphoreType.DMA
    attended, row_lse, sink_mass, totals = pl.pallas_call(
        functools.partial(kernel, zs),
        out_shape=(
            jax.ShapeDtypeStruct((ROWS, 2 * HALF), bf16),
            jax.ShapeDtypeStruct((2 * GROUP, ROWS), f32),
            jax.ShapeDtypeStruct((2 * GROUP, ROWS), f32),
            jax.ShapeDtypeStruct((1, D), f32),
        ),
        in_specs=[vmem, vmem, vmem, smem, smem],
        out_specs=(vmem, vmem, vmem, vmem),
        scratch_shapes=[
            pltpu.VMEM((zs, 2, 2, ROWS, D), bf16),
            pltpu.VMEM((2, ROWS, D), bf16),
            pltpu.VMEM((4, ROWS, HALF), bf16),
            pltpu.VMEM((ROWS, HALF), bf16),
            pltpu.VMEM((4, FLAT, D), f32),
            pltpu.VMEM((4, FLAT, D), f32),
            pltpu.VMEM((4, FLAT, D), f32),
            pltpu.VMEM((3, ROWS, HALF), bf16),
            pltpu.VMEM((2, ROWS, HALF), bf16),
            pltpu.VMEM((ROWS, HALF), bf16),
            pltpu.VMEM((ROWS, HALF), bf16),
            pltpu.VMEM((4, ROWS, D), f32),
            pltpu.VMEM((YS, YS, 16, ROWS), f32),
            pltpu.VMEM((zs, 1, D), f32),
            pltpu.VMEM((ROWS, D), f32),
            dma((2, fs, 2)),
            dma((2, fs + 1, 2)),
            dma,
            dma,
            dma((5,)),
            dma((5,)),
            dma((3,)),
            dma((3,)),
            dma((3,)),
            dma((3,)),
            dma((zs,)),
            dma((zs,)),
        ],
        compiler_params=pltpu.CompilerParams(
            collective_id=0, has_side_effects=True, vmem_limit_bytes=56 * 1024 * 1024
        ),
    )(queries, keys, values, doc_length, sink_pos)
    heads = 2 * GROUP
    return (attended, row_lse, sink_mass, totals[0, :heads], totals[0, heads : 2 * heads])


def solution(mesh):
    placed = (
        P(("doc", "seq"), None),
        P(("doc", "seq"), None),
        P(("doc", "seq"), None),
        P("doc"),
        P("doc"),
    )
    return jax.shard_map(
        functools.partial(body, zs=mesh.shape["seq"] // YS),
        mesh=mesh,
        in_specs=placed,
        out_specs=(
            P(("doc", "seq"), None),
            P(None, ("doc", "seq")),
            P(None, ("doc", "seq")),
            P("doc"),
            P("doc"),
        ),
        check_vma=False,
    )
```

```python
import functools

import jax
import jax.numpy as jnp
from jax import lax
from jax.experimental import pallas as pl
from jax.experimental.pallas import tpu as pltpu
from jax.sharding import PartitionSpec as P

D = 128
ROWS = 128
GROUP = 7
HALF = GROUP * D
FLAT = GROUP * ROWS
YS = 4
LOG2E = 1.4426950408889634
LN2 = 0.6931471805599453
SCALE = LOG2E * D**-0.5
NEG = -1e30
MESH = pl.DeviceIdType.MESH
TILES = ((0, 7),)
PARTS = ((0, 2), (2, 4), (4, 6), (6, 7))
OWN, PART, HEAD, DIAG = range(4)
Q_HEAD_0, Q_PART, Q_HEAD_1, Q_DIAG = 1, 2, 3, 5


def kernel(
    zs, q_ref, kv_ref, len_ref, sink_ref,
    att_ref, small_ref,
    kv, xbuf, qbuf, qsend, acc, l_acc, m_acc, obuf, rx, fin, fin_rx, statb, stats, red, wts,
    ring_send, ring_recv, x_send, x_recv, q_send, q_recv, st_send, st_recv, o_send, o_recv,
    red_send, red_recv, in_sem,
):
    fs = zs // 2
    seq = lax.axis_index("seq")
    z, y = seq // YS, seq % YS
    head = ((y + 1) // 2) % 2
    part = y // 2
    y_head = y + 1 - 2 * (y % 2)
    y_part = 3 - y
    y_diag = y_part + 1 - 2 * (y_part % 2)
    right, left = (z + 1) % zs, (z + zs - 1) % zs
    base = z * YS

    def at(zz, yy):
        return {"seq": zz * YS + yy}

    def remote(src, dst, send, recv, target):
        return pltpu.make_async_remote_copy(
            src_ref=src, dst_ref=dst, send_sem=send, recv_sem=recv, device_id=target, device_id_type=MESH
        )

    first = head == 0
    mine = y % 2
    wide = pl.multiple_of(head * HALF, D)
    wide_x = pl.multiple_of((1 - head) * HALF, D)
    into_place = [
        pltpu.make_async_copy(q_ref.at[:, pl.ds(wide_x, HALF)], qsend, in_sem.at[0]),
        pltpu.make_async_copy(q_ref.at[:, pl.ds(wide, HALF)], qbuf.at[OWN], in_sem.at[1]),
    ]
    for copy in into_place:
        copy.start()
    for i in range(2):
        lo, hi = kv_ref[:, 2 * i * D : (2 * i + 1) * D], kv_ref[:, (2 * i + 1) * D : (2 * i + 2) * D]
        kv[z, mine, i] = jnp.where(first, lo, hi)
        xbuf[i] = jnp.where(first, hi, lo)

    barrier = pltpu.get_barrier_semaphore()
    for target in (at(right, y), at(left, y), at(z, y_head), at(z, y_part), at(z, y_diag)):
        pl.semaphore_signal(barrier, inc=1, device_id=target, device_id_type=MESH)
    pl.semaphore_wait(barrier, 5)

    def hop(direction, s, c, plane, i):
        return remote(
            kv.at[plane, c, i], kv.at[plane, c, i],
            ring_send.at[direction, s, 2 * c + i], ring_recv.at[direction, s + 1, 2 * c + i],
            at(left if direction == 0 else right, y),
        )

    def arrived(direction, s, c, plane, i):
        return remote(
            kv.at[plane, c, i], kv.at[plane, c, i],
            ring_send.at[direction, s - 1, 2 * c + i], ring_recv.at[direction, s, 2 * c + i],
            at(left if direction == 0 else right, y),
        )

    def q_copy(k):
        lo, hi = slice(0, 4 * D), slice(4 * D, HALF)
        src, dst, target = (
            (qsend.at[:, lo], qbuf.at[HEAD, :, lo], y_head),
            (qsend.at[:, hi], qbuf.at[HEAD, :, hi], y_head),
            (qbuf.at[OWN], qbuf.at[PART], y_part),
            (qbuf.at[HEAD, :, lo], qbuf.at[DIAG, :, lo], y_part),
            (qbuf.at[HEAD, :, hi], qbuf.at[DIAG, :, hi], y_part),
        )[k]
        return remote(src, dst, q_send.at[k], q_recv.at[k], at(z, target))

    other = 1 - mine
    to_head = remote(xbuf, kv.at[z, mine], x_send, x_recv, at(z, y_head))
    from_head = remote(xbuf, kv.at[z, other], x_send, x_recv, at(z, y_head))
    to_head.start()
    for i in range(2):
        hop(0, 0, mine, z, i).start()
        hop(1, 0, mine, z, i).start()
    for copy in into_place:
        copy.wait()
    q_copy(0).start()
    q_copy(1).start()
    q_copy(2).start()
    from_head.wait_recv()
    for i in range(2):
        hop(0, 0, other, z, i).start()
        hop(1, 0, other, z, i).start()

    def owner(b):
        return jnp.where(b == OWN, y, jnp.where(b == PART, y_part, jnp.where(b == HEAD, y_head, y_diag)))

    def scores(b, heads, key_mat):
        lo, hi = heads
        rows = jnp.concatenate([qbuf[b, :, j * D : (j + 1) * D] for j in range(lo, hi)], axis=0)
        s = lax.dot_general(rows, key_mat, (((1,), (1,)), ((), ())), preferred_element_type=jnp.float32)
        return [s[:, j : j + D] * SCALE for j in range(0, key_mat.shape[0], D)]

    def top(groups):
        best = groups[0]
        for g in groups[1:]:
            best = jnp.maximum(best, g)
        return jnp.broadcast_to(jnp.max(best, axis=1, keepdims=True), best.shape)

    def total(groups):
        out = groups[0]
        for g in groups[1:]:
            out = out + g
        return out

    def first_unit(b):
        key_mat = jnp.concatenate([kv[z, 0, 0], kv[z, 1, 0]], axis=0)
        val_mat = jnp.concatenate([kv[z, 0, 1], kv[z, 1, 1]], axis=0)
        for heads in TILES:
            n = (heads[1] - heads[0]) * ROWS
            rows = pl.ds(heads[0] * ROWS, n)
            gs = scores(b, heads, key_mat)
            row = lax.broadcasted_iota(jnp.int32, (n, D), 0) % ROWS + owner(b) * ROWS
            lane = lax.broadcasted_iota(jnp.int32, (n, D), 1) + part * (2 * ROWS)
            ok = [lane + j * D <= row for j in range(2)]
            gs = [jnp.where(o, g, 2 * NEG) for o, g in zip(ok, gs)]
            m = jnp.maximum(top(gs), NEG)
            ps = [jnp.exp2(g - m) for g in gs]
            m_acc[b, rows] = m
            l_acc[b, rows] = total(ps)
            acc[b, rows] = jnp.dot(
                jnp.concatenate(ps, axis=1).astype(jnp.bfloat16), val_mat, preferred_element_type=jnp.float32
            )

    def later_unit(b, planes):
        key_mat = jnp.concatenate([kv[p, a, 0] for p in planes for a in range(2)], axis=0)
        val_mat = jnp.concatenate([kv[p, a, 1] for p in planes for a in range(2)], axis=0)
        for heads in TILES:
            rows = pl.ds(heads[0] * ROWS, (heads[1] - heads[0]) * ROWS)
            gs = scores(b, heads, key_mat)
            old = m_acc[b, rows]
            m = jnp.maximum(old, top(gs))
            alpha = jnp.exp2(old - m)
            ps = [jnp.exp2(g - m) for g in gs]
            m_acc[b, rows] = m
            l_acc[b, rows] = l_acc[b, rows] * alpha + total(ps)
            acc[b, rows] = acc[b, rows] * alpha + jnp.dot(
                jnp.concatenate(ps, axis=1).astype(jnp.bfloat16), val_mat, preferred_element_type=jnp.float32
            )

    def unit(b, s):
        below, above = (z + zs - s) % zs, (z + s) % zs
        up = (s > 0) & (s < fs) & (z >= s)
        down = (s > 0) & (z + s >= zs)
        both = up & down

        @pl.when(s == 0)
        def _():
            first_unit(b)

        @pl.when(both)
        def _():
            later_unit(b, (below, above))

        @pl.when(up != down)
        def _():
            later_unit(b, (jnp.where(up, below, above),))

    lane_id = lax.broadcasted_iota(jnp.int32, (ROWS, D), 1)

    def sink_pass(b):
        spot = lax.broadcasted_iota(jnp.int32, (ROWS, D), 1)
        hit = spot == sink_ref[0]
        for n in range(1, 4):
            hit = hit | (spot == sink_ref[n])
        row = lax.broadcasted_iota(jnp.int32, (ROWS, D), 0) + base * ROWS + owner(b) * ROWS
        hit = hit & (spot <= row)
        out = jnp.zeros((ROWS, D), jnp.float32)
        key_mat = kv[0, 0, 0]
        for heads in TILES:
            (s,) = scores(b, heads, key_mat)
            for j in range(heads[1] - heads[0]):
                g = jnp.where(hit, s[j * ROWS : (j + 1) * ROWS], 2 * NEG)
                m = jnp.max(g, axis=1, keepdims=True)
                r = m + jnp.log2(jnp.sum(jnp.exp2(g - m), axis=1, keepdims=True))
                out = jnp.where(lane_id == 8 + heads[0] + j, r, out)
        statb[b] = out

    reach = jnp.where(z < fs, z, zs - z)
    early = min(max(2 * fs - 4, Q_DIAG), 2 * fs - 1)
    sink_half = jnp.where(2 * reach - 1 <= early, early, 2 * fs - 1)

    def count(b, h):
        own = 1 + (h + 1) // 2
        late = 1 + h // 2
        begun = lambda start, cap: jnp.minimum(cap, jnp.maximum(0, 2 * (h + 1 - start)))
        last = h >= 2 * fs - 1
        n = jnp.where(
            b == OWN, jnp.where(h < 0, 0, own),
            jnp.where(b == PART, begun(Q_PART, own), jnp.where(b == HEAD, begun(Q_HEAD_1, late), begun(Q_DIAG, late))),
        )
        return jnp.where(last, fs + 1, n)

    q_head_0, q_part, q_head_1, q_diag = (min(t, 2 * fs - 1) for t in (Q_HEAD_0, Q_PART, Q_HEAD_1, Q_DIAG))

    def half_step(h, carry):
        s = 1 + h // 2
        c = (mine + h) % 2
        ahead, behind = (z + s) % zs, (z + zs - s) % zs
        for i in range(2):
            arrived(0, s, c, ahead, i).wait_recv()

            @pl.when(s < fs)
            def _():
                hop(0, s, c, ahead, i).start()

                arrived(1, s, c, behind, i).wait_recv()

            @pl.when(s < fs - 1)
            def _():
                hop(1, s, c, behind, i).start()

        @pl.when(h == q_head_0)
        def _():
            q_copy(0).wait_recv()
            q_copy(3).start()

        @pl.when(h == q_part)
        def _():
            q_copy(2).wait_recv()

        @pl.when(h == q_head_1)
        def _():
            q_copy(1).wait_recv()
            q_copy(4).start()

        @pl.when(h == q_diag)
        def _():
            q_copy(3).wait_recv()
            q_copy(4).wait_recv()

        def block(i, carry):
            b = 3 - i
            lo = jnp.where(h == 0, 0, count(b, h - 1))

            def one(u, carry):
                unit(b, u)
                return carry

            return lax.fori_loop(lo, count(b, h), one, carry)

        lax.fori_loop(0, 4, block, 0)

        @pl.when((h == sink_half) & (part == 0))
        def _():
            def one(b, carry):
                sink_pass(b)
                return carry

            lax.fori_loop(0, 4, one, 0)

        return carry

    @pl.when(part != 0)
    def _():
        statb[...] = jnp.zeros_like(statb)

    lax.fori_loop(0, 2 * fs, half_step, 0)

    def norm(b, carry):
        out = statb[b]
        for j in range(GROUP):
            rows = pl.ds(j * ROWS, ROWS)
            l = jnp.sum(l_acc[b, rows], axis=1, keepdims=True)
            r = jnp.where(l > 0, m_acc[b, rows] + jnp.log2(l), NEG)
            out = jnp.where(lane_id == j, r, out)
            l_acc[b, rows] = jnp.broadcast_to(jnp.where(l > 0, 1.0 / l, 0.0), (ROWS, D))
        out = jnp.where((lane_id % 8 == 7) | (lane_id >= 16), 0.0, out)
        stats[y, owner(b)] = out.T[:16]
        return carry

    lax.fori_loop(0, 4, norm, 0)

    def stat_copy(k, sender):
        target = (y_head, y_part, y_diag)[k]
        return remote(stats.at[sender], stats.at[sender], st_send.at[k], st_recv.at[k], at(z, target))

    def out_block(b, i):
        for j in range(GROUP):
            rows = pl.ds(j * ROWS, ROWS)
            obuf[i, :, j * D : (j + 1) * D] = (acc[b, rows] * l_acc[b, rows]).astype(jnp.bfloat16)

    def o_copy(k, n):
        lanes = slice(PARTS[n][0] * D, PARTS[n][1] * D)
        src, dst, target = (
            (obuf.at[0, :, lanes], rx.at[0, :, lanes], y_part),
            (obuf.at[1, :, lanes], rx.at[1, :, lanes], y_part),
            (fin.at[:, lanes], fin_rx.at[:, lanes], y_head),
        )[k]
        return remote(src, dst, o_send.at[k, n], o_recv.at[k, n], at(z, target))

    pieces = range(len(PARTS))
    out_block(DIAG, 0)
    for k in (1, 0, 2):
        stat_copy(k, y).start()
    out_block(PART, 1)
    for n in pieces:
        o_copy(0, n).start()
    for n in pieces:
        o_copy(1, n).start()
    for k, sender in enumerate((y_head, y_part, y_diag)):
        stat_copy(k, sender).wait_recv()

    length = len_ref[0]
    sums = [jnp.zeros((8, D), jnp.float32) for _ in range(4)]
    for blk in range(YS):
        pos = lax.broadcasted_iota(jnp.int32, (8, D), 1) + (base + blk) * ROWS
        live = pos < length
        for g, (a, b) in enumerate(((0, 3), (1, 2))):
            x0, x1 = stats[a, blk, 0:8], stats[b, blk, 0:8]
            m = jnp.maximum(x0, x1)
            full = m + jnp.log2(jnp.exp2(x0 - m) + jnp.exp2(x1 - m))
            mass = jnp.where(live, jnp.exp2(stats[a, blk, 8:16] - full), 0.0)
            nat = jnp.where(live, full * LN2, 0.0)
            sums[g] = sums[g] + nat
            sums[2 + g] = sums[2 + g] + mass

            @pl.when(y == blk)
            def _():
                small_ref[g * GROUP : (g + 1) * GROUP, :] = nat[:GROUP]
                small_ref[16 + g * GROUP : 16 + (g + 1) * GROUP, :] = mass[:GROUP]

    lane8 = lax.broadcasted_iota(jnp.int32, (8, D), 1)
    sub8 = lax.broadcasted_iota(jnp.int32, (8, D), 0)
    line = jnp.zeros((8, D), jnp.float32)
    for i, block_sum in enumerate(sums):
        col = jnp.where(sub8 < GROUP, jnp.sum(block_sum, axis=1, keepdims=True), 0.0)
        line = line + jnp.where(lane8 == sub8 + GROUP * i, col, 0.0)
    red[z] = jnp.sum(line, axis=0, keepdims=True)

    def weights(own):
        pos = lax.broadcasted_iota(jnp.int32, (8, D), 1) + (base + own) * ROWS
        live = pos < length
        x0 = stats[y, own, 0:8]
        x1 = stats[y_part, own, 0:8]
        m = jnp.maximum(x0, x1)
        full = m + jnp.log2(jnp.exp2(x0 - m) + jnp.exp2(x1 - m))
        return [jnp.where(live, jnp.exp2(x - full), 0.0) for x in (x0, x1)]

    pad = jnp.zeros((D - 32, D), jnp.float32)
    wts[...] = jnp.concatenate([*weights(y), *weights(y_head), pad], axis=0).T

    def red_copy(k):
        return remote(red.at[z], red.at[z], red_send.at[k], red_recv.at[z], at((z + k) % zs, y))

    def red_start(k, carry):
        red_copy(k).start()
        return carry

    lax.fori_loop(1, zs, red_start, 0)

    def merged(b, i, j, w):
        rows = pl.ds(j * ROWS, ROWS)
        mine_o = acc[b, rows] * (l_acc[b, rows] * wts[:, w + j : w + j + 1])
        their_o = rx[i, :, j * D : (j + 1) * D].astype(jnp.float32) * wts[:, w + 8 + j : w + 9 + j]
        return (mine_o + their_o).astype(jnp.bfloat16)

    for n in pieces:
        o_copy(0, n).wait_recv()
        for j in range(*PARTS[n]):
            fin[:, j * D : (j + 1) * D] = merged(HEAD, 0, j, 16)
        o_copy(2, n).start()
    for n in pieces:
        o_copy(1, n).wait_recv()
        for j in range(*PARTS[n]):
            obuf[2, :, j * D : (j + 1) * D] = merged(OWN, 1, j, 0)
    for n in pieces:
        o_copy(2, n).wait_recv()
    att_ref[:, :HALF] = jnp.where(first, obuf[2], fin_rx[...])
    att_ref[:, HALF:] = jnp.where(first, fin_rx[...], obuf[2])

    def red_wait(k, carry):
        src = (z + k) % zs
        remote(red.at[src], red.at[src], red_send.at[k], red_recv.at[src], at(src, y)).wait_recv()
        return carry

    lax.fori_loop(1, zs, red_wait, 0)
    result = red[0]
    for i in range(1, zs):
        result = result + red[i]
    result = result / length.astype(jnp.float32)
    small_ref[30:31, : 2 * GROUP] = result[:, : 2 * GROUP]
    small_ref[31:32, : 2 * GROUP] = result[:, 2 * GROUP : 4 * GROUP]

    to_head.wait_send()
    for k in range(5):
        q_copy(k).wait_send()
    for k in range(3):
        stat_copy(k, y).wait_send()
        for n in pieces:
            o_copy(k, n).wait_send()

    def drain(k, carry):
        red_copy(k).wait_send()
        return carry

    lax.fori_loop(1, zs, drain, 0)

    def ring_drain(s, carry):
        for c in range(2):
            for i in range(2):
                hop(0, s, c, (z + s) % zs, i).wait_send()

                @pl.when(s < fs - 1)
                def _():
                    hop(1, s, c, (z + zs - s) % zs, i).wait_send()

        return carry

    lax.fori_loop(0, fs, ring_drain, 0)


def spread(att_in, small_ref, att_ref, lse_ref, mass_ref, head_lse_ref, head_sink_ref):
    att_ref[...] = att_in[...]
    lse_ref[...] = small_ref[: 2 * GROUP]
    mass_ref[...] = small_ref[16 : 16 + 2 * GROUP]
    head_lse_ref[...] = small_ref[30:31, : 2 * GROUP]
    head_sink_ref[...] = small_ref[31:32, : 2 * GROUP]


def body(queries, keys, values, doc_length, sink_pos, zs):
    vmem = pl.BlockSpec(memory_space=pltpu.VMEM)
    smem = pl.BlockSpec(memory_space=pltpu.SMEM)
    hbm = pl.BlockSpec(memory_space=pltpu.HBM)
    fs = zs // 2
    bf16, f32 = jnp.bfloat16, jnp.float32
    dma = pltpu.SemaphoreType.DMA
    attended, small = pl.pallas_call(
        functools.partial(kernel, zs),
        out_shape=(
            jax.ShapeDtypeStruct((ROWS, 2 * HALF), bf16),
            jax.ShapeDtypeStruct((32, ROWS), f32),
        ),
        in_specs=[hbm, vmem, smem, smem],
        out_specs=(vmem, vmem),
        scratch_shapes=[
            pltpu.VMEM((zs, 2, 2, ROWS, D), bf16),
            pltpu.VMEM((2, ROWS, D), bf16),
            pltpu.VMEM((4, ROWS, HALF), bf16),
            pltpu.VMEM((ROWS, HALF), bf16),
            pltpu.VMEM((4, FLAT, D), f32),
            pltpu.VMEM((4, FLAT, D), f32),
            pltpu.VMEM((4, FLAT, D), f32),
            pltpu.VMEM((3, ROWS, HALF), bf16),
            pltpu.VMEM((2, ROWS, HALF), bf16),
            pltpu.VMEM((ROWS, HALF), bf16),
            pltpu.VMEM((ROWS, HALF), bf16),
            pltpu.VMEM((4, ROWS, D), f32),
            pltpu.VMEM((YS, YS, 16, ROWS), f32),
            pltpu.VMEM((zs, 1, D), f32),
            pltpu.VMEM((ROWS, D), f32),
            dma((2, fs, 4)),
            dma((2, fs + 1, 4)),
            dma,
            dma,
            dma((5,)),
            dma((5,)),
            dma((3,)),
            dma((3,)),
            dma((3, len(PARTS))),
            dma((3, len(PARTS))),
            dma((zs,)),
            dma((zs,)),
            dma((2,)),
        ],
        compiler_params=pltpu.CompilerParams(
            collective_id=0, has_side_effects=True, vmem_limit_bytes=53 * 1024 * 1024 + 192 * 1024
        ),
    )(queries, jnp.concatenate([keys, values], axis=1), doc_length, sink_pos)
    heads = 2 * GROUP
    attended, row_lse, sink_mass, head_lse, head_sink = pl.pallas_call(
        spread,
        out_shape=(
            jax.ShapeDtypeStruct((ROWS, 2 * HALF), bf16),
            jax.ShapeDtypeStruct((heads, ROWS), f32),
            jax.ShapeDtypeStruct((heads, ROWS), f32),
            jax.ShapeDtypeStruct((1, heads), f32),
            jax.ShapeDtypeStruct((1, heads), f32),
        ),
        in_specs=[vmem, vmem],
        out_specs=(vmem,) * 5,
        compiler_params=pltpu.CompilerParams(vmem_limit_bytes=4 * 1024 * 1024),
    )(attended, small)
    return (attended, row_lse, sink_mass, head_lse[0], head_sink[0])


def solution(mesh):
    placed = (
        P(("doc", "seq"), None),
        P(("doc", "seq"), None),
        P(("doc", "seq"), None),
        P("doc"),
        P("doc"),
    )
    return jax.shard_map(
        functools.partial(body, zs=mesh.shape["seq"] // YS),
        mesh=mesh,
        in_specs=placed,
        out_specs=(
            P(("doc", "seq"), None),
            P(None, ("doc", "seq")),
            P(None, ("doc", "seq")),
            P("doc"),
            P("doc"),
        ),
        check_vma=False,
    )
```

```python
import functools

import jax
import jax.numpy as jnp
from jax import lax
from jax.experimental import pallas as pl
from jax.experimental.pallas import tpu as pltpu
from jax.sharding import PartitionSpec as P

D = 128
ROWS = 128
GROUP = 7
HALF = GROUP * D
FLAT = GROUP * ROWS
YS = 4
LOG2E = 1.4426950408889634
LN2 = 0.6931471805599453
SCALE = LOG2E * D**-0.5
NEG = -1e30
MESH = pl.DeviceIdType.MESH
TILES = ((0, 7),)
PARTS = ((0, 2), (2, 4), (4, 6), (6, 7))
OWN, PART, HEAD, DIAG = range(4)
Q_HEAD_0, Q_PART, Q_HEAD_1, Q_DIAG = 3, 5, 7, 11


def kernel(
    zs, q_ref, kv_ref, len_ref, sink_ref,
    att_ref, small_ref,
    kv, xbuf, qbuf, qsend, acc, l_acc, m_acc, obuf, rx, fin, fin_rx, stats, red, wts,
    ring_send, ring_recv, x_send, x_recv, q_send, q_recv, st_send, st_recv, o_send, o_recv,
    red_send, red_recv, in_sem,
):
    fs = zs // 2
    seq = lax.axis_index("seq")
    z, y = seq // YS, seq % YS
    head = ((y + 1) // 2) % 2
    part = y // 2
    y_head = y + 1 - 2 * (y % 2)
    y_part = 3 - y
    y_diag = y_part + 1 - 2 * (y_part % 2)
    right, left = (z + 1) % zs, (z + zs - 1) % zs
    base = z * YS

    def at(zz, yy):
        return {"seq": zz * YS + yy}

    def remote(src, dst, send, recv, target):
        return pltpu.make_async_remote_copy(
            src_ref=src, dst_ref=dst, send_sem=send, recv_sem=recv, device_id=target, device_id_type=MESH
        )

    first = head == 0
    mine = y % 2
    wide = pl.multiple_of(head * HALF, D)
    wide_x = pl.multiple_of((1 - head) * HALF, D)
    into_place = [
        pltpu.make_async_copy(q_ref.at[:, pl.ds(wide_x, HALF)], qsend, in_sem.at[0]),
        pltpu.make_async_copy(q_ref.at[:, pl.ds(wide, HALF)], qbuf.at[OWN], in_sem.at[1]),
    ]
    for copy in into_place:
        copy.start()
    for i in range(2):
        lo, hi = kv_ref[:, 2 * i * D : (2 * i + 1) * D], kv_ref[:, (2 * i + 1) * D : (2 * i + 2) * D]
        kv[z, mine, i] = jnp.where(first, lo, hi)
        xbuf[i] = jnp.where(first, hi, lo)

    barrier = pltpu.get_barrier_semaphore()
    for target in (at(right, y), at(left, y), at(z, y_head), at(z, y_part), at(z, y_diag)):
        pl.semaphore_signal(barrier, inc=1, device_id=target, device_id_type=MESH)
    pl.semaphore_wait(barrier, 5)

    def hop(direction, s, c, plane, i):
        return remote(
            kv.at[plane, c, i], kv.at[plane, c, i],
            ring_send.at[direction, s, 2 * c + i], ring_recv.at[direction, s + 1, 2 * c + i],
            at(left if direction == 0 else right, y),
        )

    def arrived(direction, s, c, plane, i):
        return remote(
            kv.at[plane, c, i], kv.at[plane, c, i],
            ring_send.at[direction, s - 1, 2 * c + i], ring_recv.at[direction, s, 2 * c + i],
            at(left if direction == 0 else right, y),
        )

    def q_copy(k):
        lo, hi = slice(0, 4 * D), slice(4 * D, HALF)
        src, dst, target = (
            (qsend.at[:, lo], qbuf.at[HEAD, :, lo], y_head),
            (qsend.at[:, hi], qbuf.at[HEAD, :, hi], y_head),
            (qbuf.at[OWN], qbuf.at[PART], y_part),
            (qbuf.at[HEAD, :, lo], qbuf.at[DIAG, :, lo], y_part),
            (qbuf.at[HEAD, :, hi], qbuf.at[DIAG, :, hi], y_part),
        )[k]
        return remote(src, dst, q_send.at[k], q_recv.at[k], at(z, target))

    other = 1 - mine
    to_head = remote(xbuf, kv.at[z, mine], x_send, x_recv, at(z, y_head))
    from_head = remote(xbuf, kv.at[z, other], x_send, x_recv, at(z, y_head))
    to_head.start()
    for i in range(2):
        hop(0, 0, mine, z, i).start()
        hop(1, 0, mine, z, i).start()
    for copy in into_place:
        copy.wait()
    q_copy(0).start()
    q_copy(1).start()
    q_copy(2).start()
    from_head.wait_recv()
    for i in range(2):
        hop(0, 0, other, z, i).start()
        hop(1, 0, other, z, i).start()

    def owner(b):
        return jnp.where(b == OWN, y, jnp.where(b == PART, y_part, jnp.where(b == HEAD, y_head, y_diag)))

    def scores(b, heads, key_mat):
        lo, hi = heads
        rows = jnp.concatenate([qbuf[b, :, j * D : (j + 1) * D] for j in range(lo, hi)], axis=0)
        s = lax.dot_general(rows, key_mat, (((1,), (1,)), ((), ())), preferred_element_type=jnp.float32)
        return [s[:, j : j + D] for j in range(0, key_mat.shape[0], D)]

    def top(groups):
        best = groups[0]
        for g in groups[1:]:
            best = jnp.maximum(best, g)
        return jnp.broadcast_to(jnp.max(best, axis=1, keepdims=True), best.shape)

    def total(groups):
        out = groups[0]
        for g in groups[1:]:
            out = out + g
        return out

    def first_unit(b):
        key_mat = jnp.concatenate([kv[z, 0, 0], kv[z, 1, 0]], axis=0)
        val_mat = jnp.concatenate([kv[z, 0, 1], kv[z, 1, 1]], axis=0)
        for heads in TILES:
            n = (heads[1] - heads[0]) * ROWS
            rows = pl.ds(heads[0] * ROWS, n)
            gs = scores(b, heads, key_mat)
            row = lax.broadcasted_iota(jnp.int32, (n, D), 0) % ROWS + owner(b) * ROWS
            lane = lax.broadcasted_iota(jnp.int32, (n, D), 1) + part * (2 * ROWS)
            ok = [lane + j * D <= row for j in range(2)]
            gs = [jnp.where(o, g * SCALE, 2 * NEG) for o, g in zip(ok, gs)]
            m = jnp.maximum(top(gs), NEG)
            ps = [jnp.exp2(g - m) for g in gs]
            m_acc[b, rows] = m
            l_acc[b, rows] = total(ps)
            acc[b, rows] = jnp.dot(
                jnp.concatenate(ps, axis=1).astype(jnp.bfloat16), val_mat, preferred_element_type=jnp.float32
            )

    def later_unit(b, planes):
        key_mat = jnp.concatenate([kv[p, a, 0] for p in planes for a in range(2)], axis=0)
        val_mat = jnp.concatenate([kv[p, a, 1] for p in planes for a in range(2)], axis=0)
        for heads in TILES:
            rows = pl.ds(heads[0] * ROWS, (heads[1] - heads[0]) * ROWS)
            gs = scores(b, heads, key_mat)
            old = m_acc[b, rows]
            m = jnp.maximum(old, top(gs) * SCALE)
            alpha = jnp.exp2(old - m)
            ps = [jnp.exp2(g * SCALE - m) for g in gs]
            m_acc[b, rows] = m
            l_acc[b, rows] = l_acc[b, rows] * alpha + total(ps)
            acc[b, rows] = acc[b, rows] * alpha + jnp.dot(
                jnp.concatenate(ps, axis=1).astype(jnp.bfloat16), val_mat, preferred_element_type=jnp.float32
            )

    def unit(b, s):
        below, above = (z + zs - s) % zs, (z + s) % zs
        up = (s > 0) & (s < fs) & (z >= s)
        down = (s > 0) & (z + s >= zs)
        both = up & down

        @pl.when(s == 0)
        def _():
            first_unit(b)

        @pl.when(both)
        def _():
            later_unit(b, (below, above))

        @pl.when(up != down)
        def _():
            later_unit(b, (jnp.where(up, below, above),))

    lane_id = lax.broadcasted_iota(jnp.int32, (ROWS, D), 1)

    def sink_keys():
        row = lax.broadcasted_iota(jnp.int32, (16, D), 0)
        spot = lax.broadcasted_iota(jnp.int32, (16, D), 1)
        where = jnp.full((16, D), 1 << 20, jnp.int32)
        for n in range(4):
            where = jnp.where(row == n, sink_ref[n], where)
        pick = jnp.where(spot == where, 1.0, 0.0).astype(jnp.bfloat16)
        keys = jnp.dot(pick, kv[0, 0, 0], preferred_element_type=jnp.float32)
        return keys.astype(jnp.bfloat16), where

    def sink_pass(b, key_mat, where):
        rows = jnp.concatenate([qbuf[b, :, j * D : (j + 1) * D] for j in range(GROUP)], axis=0)
        s = lax.dot_general(key_mat, rows, (((1,), (1,)), ((), ())), preferred_element_type=jnp.float32)
        pos = lax.broadcasted_iota(jnp.int32, (16, D), 1) + (base + owner(b)) * ROWS
        for j in range(GROUP):
            g = jnp.where(where <= pos, s[:, j * D : (j + 1) * D] * SCALE, 2 * NEG)
            m = jnp.max(g, axis=0, keepdims=True)
            stats[y, owner(b), 8 + j : 9 + j, :] = m + jnp.log2(jnp.sum(jnp.exp2(g - m), axis=0, keepdims=True))

    reach = jnp.where(z < fs, z, zs - z)
    last = 4 * fs - 1
    early = min(max(4 * fs - 8, Q_DIAG), last)
    sink_step = jnp.minimum(jnp.maximum(4 * reach, early), last)

    def count(b, k):
        begin = jnp.where(b == OWN, 0, jnp.where(b == PART, q_part, jnp.where(b == HEAD, q_head_1, q_diag)))
        n = jnp.minimum(1 + jnp.maximum(k + 1 - b, 0) // 4, jnp.maximum(k + 1 - begin, 0))
        return jnp.where(k >= last, fs + 1, n)

    q_head_0, q_part, q_head_1, q_diag = (min(t, last) for t in (Q_HEAD_0, Q_PART, Q_HEAD_1, Q_DIAG))

    def quarter_step(k, carry):
        s = 1 + k // 4
        c = (mine + (k % 4) // 2) % 2
        i = k % 2
        ahead, behind = (z + s) % zs, (z + zs - s) % zs
        arrived(0, s, c, ahead, i).wait_recv()

        @pl.when(s < fs)
        def _():
            hop(0, s, c, ahead, i).start()

            arrived(1, s, c, behind, i).wait_recv()

        @pl.when(s < fs - 1)
        def _():
            hop(1, s, c, behind, i).start()

        @pl.when(k == q_head_0)
        def _():
            q_copy(0).wait_recv()
            q_copy(3).start()

        @pl.when(k == q_part)
        def _():
            q_copy(2).wait_recv()

        @pl.when(k == q_head_1)
        def _():
            q_copy(1).wait_recv()
            q_copy(4).start()

        @pl.when(k == q_diag)
        def _():
            q_copy(3).wait_recv()
            q_copy(4).wait_recv()

        def block(i, carry):
            b = 3 - i
            lo = jnp.where(k == 0, 0, count(b, k - 1))

            def one(u, carry):
                unit(b, u)
                return carry

            return lax.fori_loop(lo, count(b, k), one, carry)

        lax.fori_loop(0, 4, block, 0)

        @pl.when((k == sink_step) & (part == 0))
        def _():
            key_mat, where = sink_keys()

            def one(b, carry):
                sink_pass(b, key_mat, where)
                return carry

            lax.fori_loop(0, 4, one, 0)

        return carry

    stats[y] = jnp.zeros((YS, 16, ROWS), jnp.float32)

    lax.fori_loop(0, 4 * fs, quarter_step, 0)

    def norm(b, carry):
        out = jnp.zeros((ROWS, D), jnp.float32)
        for j in range(GROUP):
            rows = pl.ds(j * ROWS, ROWS)
            l = jnp.sum(l_acc[b, rows], axis=1, keepdims=True)
            r = jnp.where(l > 0, m_acc[b, rows] + jnp.log2(l), NEG)
            out = jnp.where(lane_id == j, r, out)
            l_acc[b, rows] = jnp.broadcast_to(jnp.where(l > 0, 1.0 / l, 0.0), (ROWS, D))
        stats[y, owner(b), :8, :] = out.T[:8]
        return carry

    lax.fori_loop(0, 4, norm, 0)

    def stat_copy(k, sender):
        target = (y_head, y_part, y_diag)[k]
        return remote(stats.at[sender], stats.at[sender], st_send.at[k], st_recv.at[k], at(z, target))

    def out_block(b, i):
        for j in range(GROUP):
            rows = pl.ds(j * ROWS, ROWS)
            obuf[i, :, j * D : (j + 1) * D] = (acc[b, rows] * l_acc[b, rows]).astype(jnp.bfloat16)

    def o_copy(k, n):
        lanes = slice(PARTS[n][0] * D, PARTS[n][1] * D)
        src, dst, target = (
            (obuf.at[0, :, lanes], rx.at[0, :, lanes], y_part),
            (obuf.at[1, :, lanes], rx.at[1, :, lanes], y_part),
            (fin.at[:, lanes], fin_rx.at[:, lanes], y_head),
        )[k]
        return remote(src, dst, o_send.at[k, n], o_recv.at[k, n], at(z, target))

    pieces = range(len(PARTS))
    for k in (2, 1, 0):
        stat_copy(k, y).start()
    out_block(DIAG, 0)
    out_block(PART, 1)
    for n in pieces:
        o_copy(0, n).start()
    for n in pieces:
        o_copy(1, n).start()
    for k, sender in enumerate((y_head, y_part, y_diag)):
        stat_copy(k, sender).wait_recv()

    length = len_ref[0]
    sums = [jnp.zeros((8, D), jnp.float32) for _ in range(4)]
    for blk in range(YS):
        pos = lax.broadcasted_iota(jnp.int32, (8, D), 1) + (base + blk) * ROWS
        live = pos < length
        for g, (a, b) in enumerate(((0, 3), (1, 2))):
            x0, x1 = stats[a, blk, 0:8], stats[b, blk, 0:8]
            m = jnp.maximum(x0, x1)
            full = m + jnp.log2(jnp.exp2(x0 - m) + jnp.exp2(x1 - m))
            mass = jnp.where(live, jnp.exp2(stats[a, blk, 8:16] - full), 0.0)
            nat = jnp.where(live, full * LN2, 0.0)
            sums[g] = sums[g] + nat
            sums[2 + g] = sums[2 + g] + mass

            @pl.when(y == blk)
            def _():
                small_ref[g * GROUP : (g + 1) * GROUP, :] = nat[:GROUP]
                small_ref[16 + g * GROUP : 16 + (g + 1) * GROUP, :] = mass[:GROUP]

    lane8 = lax.broadcasted_iota(jnp.int32, (8, D), 1)
    sub8 = lax.broadcasted_iota(jnp.int32, (8, D), 0)
    line = jnp.zeros((8, D), jnp.float32)
    for i, block_sum in enumerate(sums):
        col = jnp.where(sub8 < GROUP, jnp.sum(block_sum, axis=1, keepdims=True), 0.0)
        line = line + jnp.where(lane8 == sub8 + GROUP * i, col, 0.0)
    red[z] = jnp.sum(line, axis=0, keepdims=True)

    def weights(own):
        pos = lax.broadcasted_iota(jnp.int32, (8, D), 1) + (base + own) * ROWS
        live = pos < length
        x0 = stats[y, own, 0:8]
        x1 = stats[y_part, own, 0:8]
        m = jnp.maximum(x0, x1)
        full = m + jnp.log2(jnp.exp2(x0 - m) + jnp.exp2(x1 - m))
        return [jnp.where(live, jnp.exp2(x - full), 0.0) for x in (x0, x1)]

    pad = jnp.zeros((D - 32, D), jnp.float32)
    wts[...] = jnp.concatenate([*weights(y), *weights(y_head), pad], axis=0).T

    def red_copy(k):
        return remote(red.at[z], red.at[z], red_send.at[k], red_recv.at[z], at((z + k) % zs, y))

    def red_start(n, carry):
        red_copy(fs + (2 * (n % 2) - 1) * ((n + 1) // 2)).start()
        return carry

    lax.fori_loop(0, zs - 1, red_start, 0)

    def merged(b, i, j, w):
        rows = pl.ds(j * ROWS, ROWS)
        mine_o = acc[b, rows] * (l_acc[b, rows] * wts[:, w + j : w + j + 1])
        their_o = rx[i, :, j * D : (j + 1) * D].astype(jnp.float32) * wts[:, w + 8 + j : w + 9 + j]
        return (mine_o + their_o).astype(jnp.bfloat16)

    for n in pieces:
        o_copy(0, n).wait_recv()
        for j in range(*PARTS[n]):
            fin[:, j * D : (j + 1) * D] = merged(HEAD, 0, j, 16)
        o_copy(2, n).start()
    for n in pieces:
        o_copy(1, n).wait_recv()
        for j in range(*PARTS[n]):
            obuf[2, :, j * D : (j + 1) * D] = merged(OWN, 1, j, 0)
    for n in pieces:
        o_copy(2, n).wait_recv()
    att_ref[:, :HALF] = jnp.where(first, obuf[2], fin_rx[...])
    att_ref[:, HALF:] = jnp.where(first, fin_rx[...], obuf[2])

    def red_wait(k, carry):
        src = (z + k) % zs
        remote(red.at[src], red.at[src], red_send.at[k], red_recv.at[src], at(src, y)).wait_recv()
        return carry

    lax.fori_loop(1, zs, red_wait, 0)
    result = red[0]
    for i in range(1, zs):
        result = result + red[i]
    result = result / length.astype(jnp.float32)
    small_ref[30:31, : 2 * GROUP] = result[:, : 2 * GROUP]
    small_ref[31:32, : 2 * GROUP] = result[:, 2 * GROUP : 4 * GROUP]

    to_head.wait_send()
    for k in range(5):
        q_copy(k).wait_send()
    for k in range(3):
        stat_copy(k, y).wait_send()
        for n in pieces:
            o_copy(k, n).wait_send()

    def drain(k, carry):
        red_copy(k).wait_send()
        return carry

    lax.fori_loop(1, zs, drain, 0)

    def ring_drain(s, carry):
        for c in range(2):
            for i in range(2):
                hop(0, s, c, (z + s) % zs, i).wait_send()

                @pl.when(s < fs - 1)
                def _():
                    hop(1, s, c, (z + zs - s) % zs, i).wait_send()

        return carry

    lax.fori_loop(0, fs, ring_drain, 0)


def spread(att_in, small_ref, att_ref, lse_ref, mass_ref, head_lse_ref, head_sink_ref):
    att_ref[...] = att_in[...]
    lse_ref[...] = small_ref[: 2 * GROUP]
    mass_ref[...] = small_ref[16 : 16 + 2 * GROUP]
    head_lse_ref[...] = small_ref[30:31, : 2 * GROUP]
    head_sink_ref[...] = small_ref[31:32, : 2 * GROUP]


def body(queries, keys, values, doc_length, sink_pos, zs):
    vmem = pl.BlockSpec(memory_space=pltpu.VMEM)
    smem = pl.BlockSpec(memory_space=pltpu.SMEM)
    hbm = pl.BlockSpec(memory_space=pltpu.HBM)
    fs = zs // 2
    bf16, f32 = jnp.bfloat16, jnp.float32
    dma = pltpu.SemaphoreType.DMA
    attended, small = pl.pallas_call(
        functools.partial(kernel, zs),
        out_shape=(
            jax.ShapeDtypeStruct((ROWS, 2 * HALF), bf16),
            jax.ShapeDtypeStruct((32, ROWS), f32),
        ),
        in_specs=[hbm, vmem, smem, smem],
        out_specs=(vmem, vmem),
        scratch_shapes=[
            pltpu.VMEM((zs, 2, 2, ROWS, D), bf16),
            pltpu.VMEM((2, ROWS, D), bf16),
            pltpu.VMEM((4, ROWS, HALF), bf16),
            pltpu.VMEM((ROWS, HALF), bf16),
            pltpu.VMEM((4, FLAT, D), f32),
            pltpu.VMEM((4, FLAT, D), f32),
            pltpu.VMEM((4, FLAT, D), f32),
            pltpu.VMEM((3, ROWS, HALF), bf16),
            pltpu.VMEM((2, ROWS, HALF), bf16),
            pltpu.VMEM((ROWS, HALF), bf16),
            pltpu.VMEM((ROWS, HALF), bf16),
            pltpu.VMEM((YS, YS, 16, ROWS), f32),
            pltpu.VMEM((zs, 1, D), f32),
            pltpu.VMEM((ROWS, D), f32),
            dma((2, fs, 4)),
            dma((2, fs + 1, 4)),
            dma,
            dma,
            dma((5,)),
            dma((5,)),
            dma((3,)),
            dma((3,)),
            dma((3, len(PARTS))),
            dma((3, len(PARTS))),
            dma((zs,)),
            dma((zs,)),
            dma((2,)),
        ],
        compiler_params=pltpu.CompilerParams(
            collective_id=0, has_side_effects=True, vmem_limit_bytes=53 * 1024 * 1024 + 192 * 1024
        ),
    )(queries, jnp.concatenate([keys, values], axis=1), doc_length, sink_pos)
    heads = 2 * GROUP
    attended, row_lse, sink_mass, head_lse, head_sink = pl.pallas_call(
        spread,
        out_shape=(
            jax.ShapeDtypeStruct((ROWS, 2 * HALF), bf16),
            jax.ShapeDtypeStruct((heads, ROWS), f32),
            jax.ShapeDtypeStruct((heads, ROWS), f32),
            jax.ShapeDtypeStruct((1, heads), f32),
            jax.ShapeDtypeStruct((1, heads), f32),
        ),
        in_specs=[vmem, vmem],
        out_specs=(vmem,) * 5,
        compiler_params=pltpu.CompilerParams(vmem_limit_bytes=4 * 1024 * 1024),
    )(attended, small)
    return (attended, row_lse, sink_mass, head_lse[0], head_sink[0])


def solution(mesh):
    placed = (
        P(("doc", "seq"), None),
        P(("doc", "seq"), None),
        P(("doc", "seq"), None),
        P("doc"),
        P("doc"),
    )
    return jax.shard_map(
        functools.partial(body, zs=mesh.shape["seq"] // YS),
        mesh=mesh,
        in_specs=placed,
        out_specs=(
            P(("doc", "seq"), None),
            P(None, ("doc", "seq")),
            P(None, ("doc", "seq")),
            P("doc"),
            P("doc"),
        ),
        check_vma=False,
    )
```

```python
import functools

import jax
import jax.numpy as jnp
from jax import lax
from jax.experimental import pallas as pl
from jax.experimental.pallas import tpu as pltpu
from jax.sharding import PartitionSpec as P

D = 128
ROWS = 128
GROUP = 7
HALF = GROUP * D
FLAT = GROUP * ROWS
YS = 4
LOG2E = 1.4426950408889634
LN2 = 0.6931471805599453
SCALE = LOG2E * D**-0.5
NEG = -1e30
MESH = pl.DeviceIdType.MESH
TILES = ((0, 7),)
PARTS = ((0, 2), (2, 4), (4, 6), (6, 7))
OWN, PART, HEAD, DIAG = range(4)
Q_HEAD_0, Q_PART, Q_HEAD_1, Q_DIAG = 3, 5, 7, 11


def kernel(
    zs, q_ref, kv_ref, len_ref, sink_ref,
    att_ref, small_ref,
    kv, xbuf, qbuf, qsend, acc, l_acc, m_acc, obuf, rx, fin, fin_rx, stats, red, wts,
    ring_send, ring_recv, x_send, x_recv, q_send, q_recv, st_send, st_recv, o_send, o_recv,
    red_send, red_recv, in_sem,
):
    fs = zs // 2
    seq = lax.axis_index("seq")
    z, y = seq // YS, seq % YS
    head = ((y + 1) // 2) % 2
    part = y // 2
    y_head = y + 1 - 2 * (y % 2)
    y_part = 3 - y
    y_diag = y_part + 1 - 2 * (y_part % 2)
    right, left = (z + 1) % zs, (z + zs - 1) % zs
    base = z * YS

    def at(zz, yy):
        return {"seq": zz * YS + yy}

    def remote(src, dst, send, recv, target):
        return pltpu.make_async_remote_copy(
            src_ref=src, dst_ref=dst, send_sem=send, recv_sem=recv, device_id=target, device_id_type=MESH
        )

    first = head == 0
    mine = y % 2
    wide = pl.multiple_of(head * HALF, D)
    wide_x = pl.multiple_of((1 - head) * HALF, D)
    into_place = [
        pltpu.make_async_copy(q_ref.at[:, pl.ds(wide_x, HALF)], qsend, in_sem.at[0]),
        pltpu.make_async_copy(q_ref.at[:, pl.ds(wide, HALF)], qbuf.at[OWN], in_sem.at[1]),
    ]
    for copy in into_place:
        copy.start()
    for i in range(2):
        lo, hi = kv_ref[:, 2 * i * D : (2 * i + 1) * D], kv_ref[:, (2 * i + 1) * D : (2 * i + 2) * D]
        kv[z, mine, i] = jnp.where(first, lo, hi)
        xbuf[i] = jnp.where(first, hi, lo)

    barrier = pltpu.get_barrier_semaphore()
    for target in (at(right, y), at(left, y), at(z, y_head), at(z, y_part), at(z, y_diag)):
        pl.semaphore_signal(barrier, inc=1, device_id=target, device_id_type=MESH)
    pl.semaphore_wait(barrier, 5)

    def hop(direction, s, c, plane, i):
        return remote(
            kv.at[plane, c, i], kv.at[plane, c, i],
            ring_send.at[direction, s, 2 * c + i], ring_recv.at[direction, s + 1, 2 * c + i],
            at(left if direction == 0 else right, y),
        )

    def arrived(direction, s, c, plane, i):
        return remote(
            kv.at[plane, c, i], kv.at[plane, c, i],
            ring_send.at[direction, s - 1, 2 * c + i], ring_recv.at[direction, s, 2 * c + i],
            at(left if direction == 0 else right, y),
        )

    def q_copy(k):
        lo, hi = slice(0, 4 * D), slice(4 * D, HALF)
        src, dst, target = (
            (qsend.at[:, lo], qbuf.at[HEAD, :, lo], y_head),
            (qsend.at[:, hi], qbuf.at[HEAD, :, hi], y_head),
            (qbuf.at[OWN], qbuf.at[PART], y_part),
            (qbuf.at[HEAD, :, lo], qbuf.at[DIAG, :, lo], y_part),
            (qbuf.at[HEAD, :, hi], qbuf.at[DIAG, :, hi], y_part),
        )[k]
        return remote(src, dst, q_send.at[k], q_recv.at[k], at(z, target))

    other = 1 - mine
    to_head = remote(xbuf, kv.at[z, mine], x_send, x_recv, at(z, y_head))
    from_head = remote(xbuf, kv.at[z, other], x_send, x_recv, at(z, y_head))
    to_head.start()
    for i in range(2):
        hop(0, 0, mine, z, i).start()
        hop(1, 0, mine, z, i).start()
    for copy in into_place:
        copy.wait()
    q_copy(0).start()
    q_copy(1).start()
    q_copy(2).start()
    from_head.wait_recv()
    for i in range(2):
        hop(0, 0, other, z, i).start()
        hop(1, 0, other, z, i).start()

    def owner(b):
        return jnp.where(b == OWN, y, jnp.where(b == PART, y_part, jnp.where(b == HEAD, y_head, y_diag)))

    def scores(b, heads, key_mat):
        lo, hi = heads
        rows = jnp.concatenate([qbuf[b, :, j * D : (j + 1) * D] for j in range(lo, hi)], axis=0)
        s = lax.dot_general(rows, key_mat, (((1,), (1,)), ((), ())), preferred_element_type=jnp.float32)
        return [s[:, j : j + D] for j in range(0, key_mat.shape[0], D)]

    def top(groups):
        best = groups[0]
        for g in groups[1:]:
            best = jnp.maximum(best, g)
        return jnp.broadcast_to(jnp.max(best, axis=1, keepdims=True), best.shape)

    def total(groups):
        out = groups[0]
        for g in groups[1:]:
            out = out + g
        return out

    def first_unit(b):
        key_mat = jnp.concatenate([kv[z, 0, 0], kv[z, 1, 0]], axis=0)
        val_mat = jnp.concatenate([kv[z, 0, 1], kv[z, 1, 1]], axis=0)
        for heads in TILES:
            n = (heads[1] - heads[0]) * ROWS
            rows = pl.ds(heads[0] * ROWS, n)
            gs = scores(b, heads, key_mat)
            row = lax.broadcasted_iota(jnp.int32, (n, D), 0) % ROWS + owner(b) * ROWS
            lane = lax.broadcasted_iota(jnp.int32, (n, D), 1) + part * (2 * ROWS)
            ok = [lane + j * D <= row for j in range(2)]
            gs = [jnp.where(o, g * SCALE, 2 * NEG) for o, g in zip(ok, gs)]
            m = jnp.maximum(top(gs), NEG)
            ps = [jnp.exp2(g - m) for g in gs]
            m_acc[b, rows] = m
            l_acc[b, rows] = total(ps)
            acc[b, rows] = jnp.dot(
                jnp.concatenate(ps, axis=1).astype(jnp.bfloat16), val_mat, preferred_element_type=jnp.float32
            )

    def later_unit(b, planes):
        key_mat = jnp.concatenate([kv[p, a, 0] for p in planes for a in range(2)], axis=0)
        val_mat = jnp.concatenate([kv[p, a, 1] for p in planes for a in range(2)], axis=0)
        for heads in TILES:
            rows = pl.ds(heads[0] * ROWS, (heads[1] - heads[0]) * ROWS)
            gs = scores(b, heads, key_mat)
            old = m_acc[b, rows]
            m = jnp.maximum(old, top(gs) * SCALE)
            alpha = jnp.exp2(old - m)
            ps = [jnp.exp2(g * SCALE - m) for g in gs]
            m_acc[b, rows] = m
            l_acc[b, rows] = l_acc[b, rows] * alpha + total(ps)
            acc[b, rows] = acc[b, rows] * alpha + jnp.dot(
                jnp.concatenate(ps, axis=1).astype(jnp.bfloat16), val_mat, preferred_element_type=jnp.float32
            )

    def unit(b, s):
        below, above = (z + zs - s) % zs, (z + s) % zs
        up = (s > 0) & (s < fs) & (z >= s)
        down = (s > 0) & (z + s >= zs)
        both = up & down

        @pl.when(s == 0)
        def _():
            first_unit(b)

        @pl.when(both)
        def _():
            later_unit(b, (below, above))

        @pl.when(up != down)
        def _():
            later_unit(b, (jnp.where(up, below, above),))

    lane_id = lax.broadcasted_iota(jnp.int32, (ROWS, D), 1)

    def sink_keys():
        row = lax.broadcasted_iota(jnp.int32, (16, D), 0)
        spot = lax.broadcasted_iota(jnp.int32, (16, D), 1)
        where = jnp.full((16, D), 1 << 20, jnp.int32)
        for n in range(4):
            where = jnp.where(row == n, sink_ref[n], where)
        pick = jnp.where(spot == where, 1.0, 0.0).astype(jnp.bfloat16)
        keys = jnp.dot(pick, kv[0, 0, 0], preferred_element_type=jnp.float32)
        return keys.astype(jnp.bfloat16), where

    def sink_pass(b, key_mat, where):
        rows = jnp.concatenate([qbuf[b, :, j * D : (j + 1) * D] for j in range(GROUP)], axis=0)
        s = lax.dot_general(key_mat, rows, (((1,), (1,)), ((), ())), preferred_element_type=jnp.float32)
        pos = lax.broadcasted_iota(jnp.int32, (16, D), 1) + (base + owner(b)) * ROWS
        for j in range(GROUP):
            g = jnp.where(where <= pos, s[:, j * D : (j + 1) * D] * SCALE, 2 * NEG)
            m = jnp.max(g, axis=0, keepdims=True)
            stats[y, owner(b), 8 + j : 9 + j, :] = m + jnp.log2(jnp.sum(jnp.exp2(g - m), axis=0, keepdims=True))

    reach = jnp.where(z < fs, z, zs - z)
    last = 4 * fs - 1
    early = min(max(4 * fs - 8, Q_DIAG), last)
    sink_step = jnp.minimum(jnp.maximum(4 * reach, early), last)

    def count(b, k):
        begin = jnp.where(b == OWN, 0, jnp.where(b == PART, q_part, jnp.where(b == HEAD, q_head_1, q_diag)))
        n = jnp.minimum(1 + jnp.maximum(k + 1 - b, 0) // 4, jnp.maximum(k + 1 - begin, 0))
        return jnp.where(k >= last, fs + 1, n)

    q_head_0, q_part, q_head_1, q_diag = (min(t, last) for t in (Q_HEAD_0, Q_PART, Q_HEAD_1, Q_DIAG))

    def quarter_step(k, carry):
        s = 1 + k // 4
        c = (mine + (k % 4) // 2) % 2
        i = k % 2
        ahead, behind = (z + s) % zs, (z + zs - s) % zs
        arrived(0, s, c, ahead, i).wait_recv()

        @pl.when(s < fs)
        def _():
            hop(0, s, c, ahead, i).start()

            arrived(1, s, c, behind, i).wait_recv()

        @pl.when(s < fs - 1)
        def _():
            hop(1, s, c, behind, i).start()

        @pl.when(k == q_head_0)
        def _():
            q_copy(0).wait_recv()
            q_copy(3).start()

        @pl.when(k == q_part)
        def _():
            q_copy(2).wait_recv()

        @pl.when(k == q_head_1)
        def _():
            q_copy(1).wait_recv()
            q_copy(4).start()

        @pl.when(k == q_diag)
        def _():
            q_copy(3).wait_recv()
            q_copy(4).wait_recv()

        def block(i, carry):
            b = 3 - i
            lo = jnp.where(k == 0, 0, count(b, k - 1))

            def one(u, carry):
                unit(b, u)
                return carry

            return lax.fori_loop(lo, count(b, k), one, carry)

        lax.fori_loop(0, 4, block, 0)

        @pl.when((k == sink_step) & (part == 0))
        def _():
            key_mat, where = sink_keys()

            def one(b, carry):
                sink_pass(b, key_mat, where)
                return carry

            lax.fori_loop(0, 4, one, 0)

        return carry

    stats[y] = jnp.zeros((YS, 16, ROWS), jnp.float32)

    lax.fori_loop(0, 4 * fs, quarter_step, 0)

    def norm(b, carry):
        out = jnp.zeros((ROWS, D), jnp.float32)
        for j in range(GROUP):
            rows = pl.ds(j * ROWS, ROWS)
            l = jnp.sum(l_acc[b, rows], axis=1, keepdims=True)
            r = jnp.where(l > 0, m_acc[b, rows] + jnp.log2(l), NEG)
            out = jnp.where(lane_id == j, r, out)
            l_acc[b, rows] = jnp.broadcast_to(jnp.where(l > 0, 1.0 / l, 0.0), (ROWS, D))
        stats[y, owner(b), :8, :] = out.T[:8]
        return carry

    for b in range(4):
        norm(b, 0)

    def stat_copy(k, sender):
        target = (y_head, y_part, y_diag)[k]
        return remote(stats.at[sender], stats.at[sender], st_send.at[k], st_recv.at[k], at(z, target))

    def out_block(b, i):
        for j in range(GROUP):
            rows = pl.ds(j * ROWS, ROWS)
            obuf[i, :, j * D : (j + 1) * D] = (acc[b, rows] * l_acc[b, rows]).astype(jnp.bfloat16)

    def o_copy(k, n):
        lanes = slice(PARTS[n][0] * D, PARTS[n][1] * D)
        src, dst, target = (
            (obuf.at[0, :, lanes], rx.at[0, :, lanes], y_part),
            (obuf.at[1, :, lanes], rx.at[1, :, lanes], y_part),
            (fin.at[:, lanes], fin_rx.at[:, lanes], y_head),
        )[k]
        return remote(src, dst, o_send.at[k, n], o_recv.at[k, n], at(z, target))

    pieces = range(len(PARTS))
    for k in (2, 1, 0):
        stat_copy(k, y).start()
    out_block(DIAG, 0)
    out_block(PART, 1)
    for n in pieces:
        o_copy(0, n).start()
    for n in pieces:
        o_copy(1, n).start()
    for k, sender in enumerate((y_head, y_part, y_diag)):
        stat_copy(k, sender).wait_recv()

    length = len_ref[0]
    sums = [jnp.zeros((8, D), jnp.float32) for _ in range(4)]
    for blk in range(YS):
        pos = lax.broadcasted_iota(jnp.int32, (8, D), 1) + (base + blk) * ROWS
        live = pos < length
        for g, (a, b) in enumerate(((0, 3), (1, 2))):
            x0, x1 = stats[a, blk, 0:8], stats[b, blk, 0:8]
            m = jnp.maximum(x0, x1)
            full = m + jnp.log2(jnp.exp2(x0 - m) + jnp.exp2(x1 - m))
            mass = jnp.where(live, jnp.exp2(stats[a, blk, 8:16] - full), 0.0)
            nat = jnp.where(live, full * LN2, 0.0)
            sums[g] = sums[g] + nat
            sums[2 + g] = sums[2 + g] + mass

            @pl.when(y == blk)
            def _():
                small_ref[g * GROUP : (g + 1) * GROUP, :] = nat[:GROUP]
                small_ref[16 + g * GROUP : 16 + (g + 1) * GROUP, :] = mass[:GROUP]

    lane8 = lax.broadcasted_iota(jnp.int32, (8, D), 1)
    sub8 = lax.broadcasted_iota(jnp.int32, (8, D), 0)
    line = jnp.zeros((8, D), jnp.float32)
    for i, block_sum in enumerate(sums):
        col = jnp.where(sub8 < GROUP, jnp.sum(block_sum, axis=1, keepdims=True), 0.0)
        line = line + jnp.where(lane8 == sub8 + GROUP * i, col, 0.0)
    red[z] = jnp.sum(line, axis=0, keepdims=True)

    def weights(own):
        pos = lax.broadcasted_iota(jnp.int32, (8, D), 1) + (base + own) * ROWS
        live = pos < length
        x0 = stats[y, own, 0:8]
        x1 = stats[y_part, own, 0:8]
        m = jnp.maximum(x0, x1)
        full = m + jnp.log2(jnp.exp2(x0 - m) + jnp.exp2(x1 - m))
        return [jnp.where(live, jnp.exp2(x - full), 0.0) for x in (x0, x1)]

    pad = jnp.zeros((D - 32, D), jnp.float32)
    wts[...] = jnp.concatenate([*weights(y), *weights(y_head), pad], axis=0).T

    def red_copy(k):
        return remote(red.at[z], red.at[z], red_send.at[k], red_recv.at[z], at((z + k) % zs, y))

    def red_start(n, carry):
        red_copy(fs + (2 * (n % 2) - 1) * ((n + 1) // 2)).start()
        return carry

    lax.fori_loop(0, zs - 1, red_start, 0)

    def merged(b, i, j, w):
        rows = pl.ds(j * ROWS, ROWS)
        mine_o = acc[b, rows] * (l_acc[b, rows] * wts[:, w + j : w + j + 1])
        their_o = rx[i, :, j * D : (j + 1) * D].astype(jnp.float32) * wts[:, w + 8 + j : w + 9 + j]
        return (mine_o + their_o).astype(jnp.bfloat16)

    for n in pieces:
        o_copy(0, n).wait_recv()
        for j in range(*PARTS[n]):
            fin[:, j * D : (j + 1) * D] = merged(HEAD, 0, j, 16)
        o_copy(2, n).start()
    for n in pieces:
        o_copy(1, n).wait_recv()
        for j in range(*PARTS[n]):
            obuf[2, :, j * D : (j + 1) * D] = merged(OWN, 1, j, 0)
    for n in pieces:
        o_copy(2, n).wait_recv()
    att_ref[:, :HALF] = jnp.where(first, obuf[2], fin_rx[...])
    att_ref[:, HALF:] = jnp.where(first, fin_rx[...], obuf[2])

    def red_wait(k, carry):
        src = (z + k) % zs
        remote(red.at[src], red.at[src], red_send.at[k], red_recv.at[src], at(src, y)).wait_recv()
        return carry

    lax.fori_loop(1, zs, red_wait, 0)
    result = red[0]
    for i in range(1, zs):
        result = result + red[i]
    result = result / length.astype(jnp.float32)
    small_ref[30:31, : 2 * GROUP] = result[:, : 2 * GROUP]
    small_ref[31:32, : 2 * GROUP] = result[:, 2 * GROUP : 4 * GROUP]

    to_head.wait_send()
    for k in range(5):
        q_copy(k).wait_send()
    for k in range(3):
        stat_copy(k, y).wait_send()
        for n in pieces:
            o_copy(k, n).wait_send()

    def drain(k, carry):
        red_copy(k).wait_send()
        return carry

    lax.fori_loop(1, zs, drain, 0)

    def ring_drain(s, carry):
        for c in range(2):
            for i in range(2):
                hop(0, s, c, (z + s) % zs, i).wait_send()

                @pl.when(s < fs - 1)
                def _():
                    hop(1, s, c, (z + zs - s) % zs, i).wait_send()

        return carry

    lax.fori_loop(0, fs, ring_drain, 0)


def spread(att_in, small_ref, att_ref, lse_ref, mass_ref, head_lse_ref, head_sink_ref):
    att_ref[...] = att_in[...]
    lse_ref[...] = small_ref[: 2 * GROUP]
    mass_ref[...] = small_ref[16 : 16 + 2 * GROUP]
    head_lse_ref[...] = small_ref[30:31, : 2 * GROUP]
    head_sink_ref[...] = small_ref[31:32, : 2 * GROUP]


def body(queries, keys, values, doc_length, sink_pos, zs):
    vmem = pl.BlockSpec(memory_space=pltpu.VMEM)
    smem = pl.BlockSpec(memory_space=pltpu.SMEM)
    hbm = pl.BlockSpec(memory_space=pltpu.HBM)
    fs = zs // 2
    bf16, f32 = jnp.bfloat16, jnp.float32
    dma = pltpu.SemaphoreType.DMA
    attended, small = pl.pallas_call(
        functools.partial(kernel, zs),
        out_shape=(
            jax.ShapeDtypeStruct((ROWS, 2 * HALF), bf16),
            jax.ShapeDtypeStruct((32, ROWS), f32),
        ),
        in_specs=[hbm, vmem, smem, smem],
        out_specs=(vmem, vmem),
        scratch_shapes=[
            pltpu.VMEM((zs, 2, 2, ROWS, D), bf16),
            pltpu.VMEM((2, ROWS, D), bf16),
            pltpu.VMEM((4, ROWS, HALF), bf16),
            pltpu.VMEM((ROWS, HALF), bf16),
            pltpu.VMEM((4, FLAT, D), f32),
            pltpu.VMEM((4, FLAT, D), f32),
            pltpu.VMEM((4, FLAT, D), f32),
            pltpu.VMEM((3, ROWS, HALF), bf16),
            pltpu.VMEM((2, ROWS, HALF), bf16),
            pltpu.VMEM((ROWS, HALF), bf16),
            pltpu.VMEM((ROWS, HALF), bf16),
            pltpu.VMEM((YS, YS, 16, ROWS), f32),
            pltpu.VMEM((zs, 1, D), f32),
            pltpu.VMEM((ROWS, D), f32),
            dma((2, fs, 4)),
            dma((2, fs + 1, 4)),
            dma,
            dma,
            dma((5,)),
            dma((5,)),
            dma((3,)),
            dma((3,)),
            dma((3, len(PARTS))),
            dma((3, len(PARTS))),
            dma((zs,)),
            dma((zs,)),
            dma((2,)),
        ],
        compiler_params=pltpu.CompilerParams(
            collective_id=0, has_side_effects=True, vmem_limit_bytes=53 * 1024 * 1024 + 192 * 1024
        ),
    )(queries, jnp.concatenate([keys, values], axis=1), doc_length, sink_pos)
    heads = 2 * GROUP
    attended, row_lse, sink_mass, head_lse, head_sink = pl.pallas_call(
        spread,
        out_shape=(
            jax.ShapeDtypeStruct((ROWS, 2 * HALF), bf16),
            jax.ShapeDtypeStruct((heads, ROWS), f32),
            jax.ShapeDtypeStruct((heads, ROWS), f32),
            jax.ShapeDtypeStruct((1, heads), f32),
            jax.ShapeDtypeStruct((1, heads), f32),
        ),
        in_specs=[vmem, vmem],
        out_specs=(vmem,) * 5,
        compiler_params=pltpu.CompilerParams(vmem_limit_bytes=4 * 1024 * 1024),
    )(attended, small)
    return (attended, row_lse, sink_mass, head_lse[0], head_sink[0])


def solution(mesh):
    placed = (
        P(("doc", "seq"), None),
        P(("doc", "seq"), None),
        P(("doc", "seq"), None),
        P("doc"),
        P("doc"),
    )
    return jax.shard_map(
        functools.partial(body, zs=mesh.shape["seq"] // YS),
        mesh=mesh,
        in_specs=placed,
        out_specs=(
            P(("doc", "seq"), None),
            P(None, ("doc", "seq")),
            P(None, ("doc", "seq")),
            P("doc"),
            P("doc"),
        ),
        check_vma=False,
    )
```
